32 devices in a mesh: pts: 16 (over z, y, x), cand: 2 (over core).
Axes of the slice: x: 2, y: 2, z: 4, core: 2. Of those that a mesh axis runs over, the one named last changes fastest.
Arguments:
- points: bfloat16 [8192, 4096], P('pts'), may hold values from -6 to 6
- weights: float32 [8192], P('pts'), may hold values from 0.25 to 4
- coverage: float32 [8192], P('pts'), may hold values from 0 to 1.5
- cand_index: int32 [2, 256], P(None, 'pts'), may hold values from 0 to 511
- winners: int32 [2], replicated, may hold values from 0 to 255
Outputs:
- gains: float32 [2, 256], P(None, ('pts', 'cand'))
- final_cover: float32 [8192], P('pts')
The draws below stay inside these ranges and needn't reach their ends.
All inputs are finite; a program needn't handle non-finite values.
Results may differ from the reference program's by a relative error of at most 0.0003.
Values may be sent and summed in bfloat16 or wider, within the bound.
A program may use at most 64 MiB of HBM per device.

```python
import math
import jax
import jax.numpy as jnp
from jax import lax

D = 4096
PTS_DEV = 512
CAND_DEV = 8
ITERS = 2
NPTS = 8192
CANDS = 256
N_PTS = 16
N_CAND = 2


def touch_ends(entries, rng, low, largest):
    longest = entries.shape.index(max(entries.shape))
    spots = []
    for shift in (0, 1):
        where = [jax.random.randint(jax.random.fold_in(rng, axis), (), 0, length) for axis, length in enumerate(entries.shape)]
        where[longest] = (where[longest] + shift) % entries.shape[longest]
        spots.append(tuple(where))
    return entries.at[spots[0]].set(low).at[spots[1]].set(largest)


def shard_levels(rng, extent, cuts, low, largest):
    factor_of = 1.0
    for position, parts in cuts:
        draws = jax.random.uniform(jax.random.fold_in(jax.random.fold_in(rng, 6), position), (parts,), jnp.float32, low / len(cuts), largest / len(cuts))
        factor_of = factor_of * jnp.repeat(jnp.exp(draws), extent[position] // parts).reshape((-1,) + (1,) * (len(extent) - 1 - position))
    return factor_of


def scatter_about(stream_key, extent, width, reach, shards=(), kind=jnp.bfloat16):
    array = width * jax.random.normal(stream_key, extent, jnp.float32)
    if shards:
        array = array * shard_levels(stream_key, extent, shards, -0.22, 0.18)
    return jnp.clip(array, -reach, reach).astype(kind)


def setup_inputs(seed: int = 0) -> dict:
    arg_keys = jax.random.split(jax.random.key(seed), 6)
    return {
        "points": scatter_about(arg_keys[0], (NPTS, D), 1.0, 6.0, ((0, 16),)),
        "weights": jnp.clip(jnp.exp(math.log(4.0) - 2.7725887 * jax.random.uniform(arg_keys[1], (NPTS,), jnp.float32) ** shard_levels(arg_keys[1], (NPTS,), ((0, 16),), -0.2, 0.2)), 0.25, 4.0),
        "coverage": jnp.clip(1.5 * jax.random.uniform(arg_keys[2], (NPTS,), jnp.float32) ** shard_levels(arg_keys[2], (NPTS,), ((0, 16),), -0.2, 0.2), 0.0, 1.5),
        "cand_index": touch_ends(jax.random.randint(arg_keys[3], (ITERS, CANDS), 0, PTS_DEV), jax.random.fold_in(arg_keys[3], 1), 0, PTS_DEV - 1).astype(jnp.int32),
        "winners": jax.random.randint(arg_keys[4], (ITERS,), 0, CANDS).astype(jnp.int32),
    }


def shard_gain(total, block, cands, scale):
    rows_blk, weight_blk, cover_blk = block
    sim = lax.dot_general(rows_blk, cands, (((1,), (1,)), ((), ())), preferred_element_type=jnp.float32) * scale
    term = jnp.sum(weight_blk[:, None] * jnp.maximum(sim - cover_blk[:, None], jnp.float32(0.0)), axis=0)
    return total + term, None


def reference(points, weights, coverage, cand_index, winners):
    scale = jnp.float32(D ** -0.5)
    per_row = CAND_DEV * N_CAND
    column = jnp.arange(CANDS, dtype=jnp.int32)
    owner = (column // per_row).astype(jnp.int32)
    rows = (owner[None, :] * PTS_DEV + cand_index).astype(jnp.int32)
    cover = coverage
    blocked_points = points.reshape(N_PTS, PTS_DEV, D)
    blocked_weights = weights.reshape(N_PTS, PTS_DEV)
    results = []
    for step in range(ITERS):
        cands = jnp.take(points, rows[step], axis=0)
        blocked_cover = cover.reshape(N_PTS, PTS_DEV)
        total, _ = lax.scan(lambda c, b: shard_gain(c, b, cands, scale), jnp.zeros((CANDS,), jnp.float32), (blocked_points, blocked_weights, blocked_cover))
        results.append(total / NPTS)
        chosen = jnp.take(points, rows[step][winners[step]][None], axis=0)
        sim = lax.dot_general(points, chosen, (((1,), (1,)), ((), ())), preferred_element_type=jnp.float32)[:, 0] * scale
        cover = jnp.maximum(cover, sim)
    return jnp.stack(results), cover
```

```python
import functools

import jax
import jax.numpy as jnp
from jax import lax
from jax.experimental import pallas as pl
from jax.experimental.pallas import tpu as pltpu
from jax.sharding import PartitionSpec as P

MESH = pl.DeviceIdType.MESH
CHUNKS = 4


def kernel(n, m, iters, per_dev, points_hbm, weight_ref, cover_ref, index_ref, winner_ref,
           gains_ref, final_ref, points, cands, sims, cols, parts, padded,
           load_sem, send_sem, recv_sem, col_send, col_recv, part_send, part_recv):
    me = lax.axis_index("pts")
    mine = lax.axis_index("cand")
    length = n // 4
    z = me // 4
    lane = me % 4
    x, y = lane % 2, lane // 2
    rows, width = points.shape
    block = iters * per_dev
    step_cols = width // CHUNKS
    scale = width ** (-0.5)

    load = pltpu.make_async_copy(points_hbm, points, load_sem)
    load.start()

    to_x = z * 4 + y * 2 + (1 - x)
    to_y = z * 4 + (1 - y) * 2 + x
    up, down = me + 4, me - 4
    has_up, has_down = z < length - 1, z > 0

    barrier = pltpu.get_barrier_semaphore()

    def greet(pts, cand):
        pl.semaphore_signal(barrier, inc=1, device_id=(pts, cand), device_id_type=MESH)

    greet(to_x, mine)
    greet(to_y, mine)
    for other in range(1, m):
        greet(me, lax.rem(mine + other, m))
    pl.when(has_up)(lambda: greet(up, mine))
    pl.when(has_down)(lambda: greet(down, mine))

    load.wait()
    place_row = lax.broadcasted_iota(jnp.int32, (block, rows), 0)
    place_col = lax.broadcasted_iota(jnp.int32, (block, rows), 1)
    choose = jnp.zeros((block, rows), jnp.float32)
    for t in range(iters):
        for k in range(per_dev):
            hit = place_col == index_ref[t, mine * per_dev + k]
            choose = jnp.where((place_row == t * per_dev + k) & hit, 1.0, choose)
    choose = choose.astype(jnp.bfloat16)
    for q in range(CHUNKS):
        span = slice(q * step_cols, (q + 1) * step_cols)
        cands[me, :, span] = jnp.dot(
            choose, points[:, span], preferred_element_type=jnp.float32).astype(jnp.bfloat16)

    pl.semaphore_wait(
        barrier, 2 + (m - 1) + has_up.astype(jnp.int32) + has_down.astype(jnp.int32))

    def columns(q):
        return pl.ds(pl.multiple_of(q * step_cols, 128), step_cols)

    def copy(p, q, way, target):
        part = cands.at[p, :, columns(q)]
        return pltpu.make_async_remote_copy(
            src_ref=part, dst_ref=part, send_sem=send_sem.at[p, way],
            recv_sem=recv_sem.at[p, q], device_id=(target, mine), device_id_type=MESH)

    last = length - 1
    is_end = (z == 0) | (z == last)

    def direct(zp):
        outer = (zp == 0) | (zp == last)
        return outer == is_end

    def routes(kind, zp):
        if kind == 0:
            return [(2, has_up & (zp <= z), up), (3, has_down & (zp >= z), down),
                    (0, None, to_x), (1, None, to_y)]
        if kind == 1:
            return [(1, direct(zp) & (zp % 2 == 1), to_y)]
        if kind == 2:
            return [(0, direct(zp) & (zp % 2 == 0), to_x)]
        inner = (zp > 0) & (zp < last)
        return [(2, (inner & (z == last - 1)) | ((zp == 0) & (z < last - 1)), up),
                (3, (inner & (z == 1)) | ((zp == last) & (z > 1)), down)]

    lanes = [lane, y * 2 + (1 - x), (1 - y) * 2 + x, (1 - y) * 2 + (1 - x)]

    def forward(kind, zp, q):
        p = zp * 4 + lanes[kind]
        for way, wanted, target in routes(kind, zp):
            def go(way=way, target=target):
                copy(p, q, way, target).start()
            if wanted is None:
                go()
            else:
                pl.when(wanted)(go)

    def settle(kind, zp):
        p = zp * 4 + lanes[kind]
        for way, wanted, target in routes(kind, zp):
            def go(way=way, target=target):
                pltpu.make_async_remote_copy(
                    src_ref=cands.at[p], dst_ref=cands.at[p], send_sem=send_sem.at[p, way],
                    recv_sem=recv_sem.at[p, 0], device_id=(target, mine),
                    device_id_type=MESH).wait_send()
            if wanted is None:
                go()
            else:
                pl.when(wanted)(go)

    for q in range(CHUNKS):
        forward(0, z, q)

    def stage(s, q):
        for kind, delay in ((3, 2), (0, 0), (1, 1), (2, 1)):
            for sign in (-1, 1):
                d = s - delay
                zp = z + sign * d
                valid = (zp >= 0) & (zp <= last) & (d >= (1 if kind == 0 or sign == 1 else 0))

                @pl.when(valid)
                def _(kind=kind, zp=zp):
                    copy(zp * 4 + lanes[kind], q, 0, to_x).wait_recv()
                    forward(kind, zp, q)

    def all_chunks(s, carry):
        lax.fori_loop(0, CHUNKS, lambda q, c: (stage(s, q), c)[1], 0)
        return carry

    lax.fori_loop(1, length + 1, all_chunks, 0)
    for q in range(CHUNKS):
        stage(length + 1, q)
        span = slice(q * step_cols, (q + 1) * step_cols)
        product = lax.dot_general(
            cands[:, :, span].reshape(n * block, step_cols), points[:, span],
            (((1,), (1,)), ((), ())), preferred_element_type=jnp.float32)
        if q == 0:
            sims[...] = product
        elif q < CHUNKS - 1:
            sims[...] += product
        else:
            sims[...] = (sims[...] + product) * scale

    def sim_of(t):
        return sims[...].reshape(n, iters, per_dev, rows)[:, t].reshape(n * per_dev, rows)

    place = lax.broadcasted_iota(jnp.int32, (n * per_dev, 1), 0)
    column = (place // per_dev) * (per_dev * m) + mine * per_dev + place % per_dev
    for t in range(iters):
        picked = jnp.where(column == winner_ref[t], sim_of(t), 0.0)
        cols[mine, t:t + 1, :] = jnp.sum(picked, axis=0, keepdims=True)

    def col_copy(slot, peer):
        return pltpu.make_async_remote_copy(
            src_ref=cols.at[slot], dst_ref=cols.at[slot], send_sem=col_send.at[peer],
            recv_sem=col_recv.at[slot], device_id=(me, peer), device_id_type=MESH)

    peers = [lax.rem(mine + other, m) for other in range(1, m)]
    for peer in peers:
        col_copy(mine, peer).start()

    weight = weight_ref[...]

    def gain(t, cover):
        terms = weight * jnp.maximum(sim_of(t) - cover, 0.0)
        folded = terms[:, 0:128]
        for g in range(1, rows // 128):
            folded = folded + terms[:, g * 128:(g + 1) * 128]
        return jnp.sum(folded.T, axis=0, keepdims=True)

    cover = cover_ref[...]
    for t in range(iters):
        parts[me, t:t + 1, :] = gain(t, cover)
        if t == 0:
            for peer in peers:
                col_copy(peer, peer).wait_recv()
        best = cols[0, t:t + 1, :]
        for c in range(1, m):
            best = best + cols[c, t:t + 1, :]
        cover = jnp.maximum(cover, best)

    def part_copy(slot, target):
        return pltpu.make_async_remote_copy(
            src_ref=parts.at[slot], dst_ref=parts.at[slot], send_sem=part_send.at[target],
            recv_sem=part_recv.at[slot], device_id=(target, mine), device_id_type=MESH)

    others = [lax.rem(me + other, n) for other in range(1, n)]
    for target in others:
        part_copy(me, target).start()
    final_ref[...] = cover

    settle(0, z)
    for kind in range(4):
        def each(zp, carry, kind=kind):
            if kind == 0:
                pl.when(zp != z)(lambda: settle(0, zp))
            else:
                settle(kind, zp)
            return carry
        lax.fori_loop(0, length, each, 0)
    for peer in peers:
        col_copy(mine, peer).wait_send()

    for source in others:
        part_copy(source, source).wait_recv()
    total = parts[0]
    for p in range(1, n):
        total = total + parts[p]
    padded[...] = jnp.zeros_like(padded)
    padded[0:iters, :] = total / float(rows * n)
    turned = pltpu.roll(padded[...], (n - me) * per_dev, 1)
    gains_ref[...] = turned[0:iters, 0:per_dev]
    for target in others:
        part_copy(me, target).wait_send()


def solution(mesh):
    n, m = mesh.shape["pts"], mesh.shape["cand"]

    def body(points, weights, coverage, cand_index, winners):
        rows, width = points.shape
        iters, per_row = cand_index.shape
        per_dev = per_row // m
        block = iters * per_dev
        vmem = pl.BlockSpec(memory_space=pltpu.VMEM)
        smem = pl.BlockSpec(memory_space=pltpu.SMEM)
        dma = pltpu.SemaphoreType.DMA
        gains, final = pl.pallas_call(
            functools.partial(kernel, n, m, iters, per_dev),
            out_shape=(jax.ShapeDtypeStruct((iters, per_dev), jnp.float32),
                       jax.ShapeDtypeStruct((1, rows), jnp.float32)),
            in_specs=[pl.BlockSpec(memory_space=pl.ANY), vmem, vmem, smem, smem],
            out_specs=(vmem, vmem),
            scratch_shapes=[
                pltpu.VMEM((rows, width), jnp.bfloat16),
                pltpu.VMEM((n, block, width), jnp.bfloat16),
                pltpu.VMEM((n * block, rows), jnp.float32),
                pltpu.VMEM((m, iters, rows), jnp.float32),
                pltpu.VMEM((n, iters, n * per_dev), jnp.float32),
                pltpu.VMEM((8, n * per_dev), jnp.float32),
                dma, dma((n, 4)), dma((n, CHUNKS)), dma((m,)), dma((m,)), dma((n,)), dma((n,)),
            ],
            compiler_params=pltpu.CompilerParams(collective_id=0, has_side_effects=True),
        )(points, weights.reshape(1, rows), coverage.reshape(1, rows), cand_index, winners)
        return gains, final.reshape(rows)

    return jax.shard_map(
        body,
        mesh=mesh,
        in_specs=(P("pts", None), P("pts"), P("pts"), P(None, "pts"), P()),
        out_specs=(P(None, ("pts", "cand")), P("pts")),
        check_vma=False,
    )
```

```python
import functools

import jax
import jax.numpy as jnp
from jax import lax
from jax.experimental import pallas as pl
from jax.experimental.pallas import tpu as pltpu
from jax.sharding import PartitionSpec as P

MESH = pl.DeviceIdType.MESH
CHUNKS = 8


def kernel(n, m, iters, per_dev, points_hbm, weight_ref, cover_ref, index_ref, winner_ref,
           gains_ref, final_ref, points, cands, sims, cols, parts, padded,
           load_sem, send_sem, recv_sem, col_send, col_recv, part_send, part_recv):
    me = lax.axis_index("pts")
    mine = lax.axis_index("cand")
    length = n // 4
    z = me // 4
    lane = me % 4
    x, y = lane % 2, lane // 2
    rows, width = points.shape
    block = iters * per_dev
    step_cols = width // CHUNKS
    scale = width ** (-0.5)

    load = pltpu.make_async_copy(points_hbm, points, load_sem)
    load.start()

    to_x = z * 4 + y * 2 + (1 - x)
    to_y = z * 4 + (1 - y) * 2 + x
    up, down = me + 4, me - 4
    has_up, has_down = z < length - 1, z > 0

    barrier = pltpu.get_barrier_semaphore()

    def greet(pts, cand):
        pl.semaphore_signal(barrier, inc=1, device_id=(pts, cand), device_id_type=MESH)

    greet(to_x, mine)
    greet(to_y, mine)
    for other in range(1, m):
        greet(me, lax.rem(mine + other, m))
    pl.when(has_up)(lambda: greet(up, mine))
    pl.when(has_down)(lambda: greet(down, mine))

    load.wait()
    place_row = lax.broadcasted_iota(jnp.int32, (block, rows), 0)
    place_col = lax.broadcasted_iota(jnp.int32, (block, rows), 1)
    choose = jnp.zeros((block, rows), jnp.float32)
    for t in range(iters):
        for k in range(per_dev):
            hit = place_col == index_ref[t, mine * per_dev + k]
            choose = jnp.where((place_row == t * per_dev + k) & hit, 1.0, choose)
    choose = choose.astype(jnp.bfloat16)
    for q in range(CHUNKS):
        span = slice(q * step_cols, (q + 1) * step_cols)
        cands[me, :, span] = jnp.dot(
            choose, points[:, span], preferred_element_type=jnp.float32).astype(jnp.bfloat16)

    pl.semaphore_wait(
        barrier, 2 + (m - 1) + has_up.astype(jnp.int32) + has_down.astype(jnp.int32))

    def columns(q):
        return pl.ds(pl.multiple_of(q * step_cols, 128), step_cols)

    def copy(p, q, way, target):
        part = cands.at[p, :, columns(q)]
        return pltpu.make_async_remote_copy(
            src_ref=part, dst_ref=part, send_sem=send_sem.at[p, way],
            recv_sem=recv_sem.at[p, q], device_id=(target, mine), device_id_type=MESH)

    last = length - 1
    middle = length // 2

    def direct(zp):
        return (zp >= middle) == (z >= middle)

    def routes(kind, zp):
        if kind == 0:
            return [(2, has_up & (zp <= z), up), (3, has_down & (zp >= z), down),
                    (0, None, to_x), (1, None, to_y)]
        if kind == 1:
            return [(1, direct(zp) & (zp % 2 == 1), to_y)]
        if kind == 2:
            return [(0, direct(zp) & (zp % 2 == 0), to_x)]
        return [(2, (zp < middle) & (z >= middle - 1) & has_up, up),
                (3, (zp >= middle) & (z <= middle) & has_down, down)]

    lanes = [lane, y * 2 + (1 - x), (1 - y) * 2 + x, (1 - y) * 2 + (1 - x)]

    def forward(kind, zp, q):
        p = zp * 4 + lanes[kind]
        for way, wanted, target in routes(kind, zp):
            def go(way=way, target=target):
                copy(p, q, way, target).start()
            if wanted is None:
                go()
            else:
                pl.when(wanted)(go)

    def settle(kind, zp):
        p = zp * 4 + lanes[kind]
        for way, wanted, target in routes(kind, zp):
            def go(way=way, target=target):
                pltpu.make_async_remote_copy(
                    src_ref=cands.at[p], dst_ref=cands.at[p], send_sem=send_sem.at[p, way],
                    recv_sem=recv_sem.at[p, 0], device_id=(target, mine),
                    device_id_type=MESH).wait_send()
            if wanted is None:
                go()
            else:
                pl.when(wanted)(go)

    for q in range(CHUNKS):
        forward(0, z, q)

    def stage(s, q):
        for kind, delay in ((3, 2), (0, 0), (1, 1), (2, 1)):
            for sign in (-1, 1):
                d = s - delay
                zp = z + sign * d
                valid = (zp >= 0) & (zp <= last) & (d >= (1 if kind == 0 or sign == 1 else 0))

                @pl.when(valid)
                def _(kind=kind, zp=zp):
                    copy(zp * 4 + lanes[kind], q, 0, to_x).wait_recv()
                    forward(kind, zp, q)

    def all_chunks(s, carry):
        lax.fori_loop(0, CHUNKS, lambda q, c: (stage(s, q), c)[1], 0)
        return carry

    lax.fori_loop(1, length + 1, all_chunks, 0)
    for q in range(CHUNKS):
        stage(length + 1, q)
        span = slice(q * step_cols, (q + 1) * step_cols)
        product = lax.dot_general(
            cands[:, :, span].reshape(n * block, step_cols), points[:, span],
            (((1,), (1,)), ((), ())), preferred_element_type=jnp.float32)
        if q == 0:
            sims[...] = product
        elif q < CHUNKS - 1:
            sims[...] += product
        else:
            sims[...] = (sims[...] + product) * scale

    def sim_of(t):
        return sims[...].reshape(n, iters, per_dev, rows)[:, t].reshape(n * per_dev, rows)

    place = lax.broadcasted_iota(jnp.int32, (n * per_dev, 1), 0)
    column = (place // per_dev) * (per_dev * m) + mine * per_dev + place % per_dev
    for t in range(iters):
        picked = jnp.where(column == winner_ref[t], sim_of(t), 0.0)
        cols[mine, t:t + 1, :] = jnp.sum(picked, axis=0, keepdims=True)

    def col_copy(slot, peer):
        return pltpu.make_async_remote_copy(
            src_ref=cols.at[slot], dst_ref=cols.at[slot], send_sem=col_send.at[peer],
            recv_sem=col_recv.at[slot], device_id=(me, peer), device_id_type=MESH)

    peers = [lax.rem(mine + other, m) for other in range(1, m)]
    for peer in peers:
        col_copy(mine, peer).start()

    weight = weight_ref[...]

    def gain(t, cover):
        terms = weight * jnp.maximum(sim_of(t) - cover, 0.0)
        folded = terms[:, 0:128]
        for g in range(1, rows // 128):
            folded = folded + terms[:, g * 128:(g + 1) * 128]
        return jnp.sum(folded.T, axis=0, keepdims=True)

    cover = cover_ref[...]
    for t in range(iters):
        parts[me, t:t + 1, :] = gain(t, cover)
        if t == 0:
            for peer in peers:
                col_copy(peer, peer).wait_recv()
        best = cols[0, t:t + 1, :]
        for c in range(1, m):
            best = best + cols[c, t:t + 1, :]
        cover = jnp.maximum(cover, best)

    def part_copy(slot, target):
        return pltpu.make_async_remote_copy(
            src_ref=parts.at[slot], dst_ref=parts.at[slot], send_sem=part_send.at[target],
            recv_sem=part_recv.at[slot], device_id=(target, mine), device_id_type=MESH)

    others = [lax.rem(me + other, n) for other in range(1, n)]
    for target in others:
        part_copy(me, target).start()
    final_ref[...] = cover

    settle(0, z)
    for kind in range(4):
        def each(zp, carry, kind=kind):
            if kind == 0:
                pl.when(zp != z)(lambda: settle(0, zp))
            else:
                settle(kind, zp)
            return carry
        lax.fori_loop(0, length, each, 0)
    for peer in peers:
        col_copy(mine, peer).wait_send()

    for source in others:
        part_copy(source, source).wait_recv()
    total = parts[0]
    for p in range(1, n):
        total = total + parts[p]
    padded[...] = jnp.zeros_like(padded)
    padded[0:iters, :] = total / float(rows * n)
    turned = pltpu.roll(padded[...], (n - me) * per_dev, 1)
    gains_ref[...] = turned[0:iters, 0:per_dev]
    for target in others:
        part_copy(me, target).wait_send()


def solution(mesh):
    n, m = mesh.shape["pts"], mesh.shape["cand"]

    def body(points, weights, coverage, cand_index, winners):
        rows, width = points.shape
        iters, per_row = cand_index.shape
        per_dev = per_row // m
        block = iters * per_dev
        vmem = pl.BlockSpec(memory_space=pltpu.VMEM)
        smem = pl.BlockSpec(memory_space=pltpu.SMEM)
        dma = pltpu.SemaphoreType.DMA
        gains, final = pl.pallas_call(
            functools.partial(kernel, n, m, iters, per_dev),
            out_shape=(jax.ShapeDtypeStruct((iters, per_dev), jnp.float32),
                       jax.ShapeDtypeStruct((1, rows), jnp.float32)),
            in_specs=[pl.BlockSpec(memory_space=pl.ANY), vmem, vmem, smem, smem],
            out_specs=(vmem, vmem),
            scratch_shapes=[
                pltpu.VMEM((rows, width), jnp.bfloat16),
                pltpu.VMEM((n, block, width), jnp.bfloat16),
                pltpu.VMEM((n * block, rows), jnp.float32),
                pltpu.VMEM((m, iters, rows), jnp.float32),
                pltpu.VMEM((n, iters, n * per_dev), jnp.float32),
                pltpu.VMEM((8, n * per_dev), jnp.float32),
                dma, dma((n, 4)), dma((n, CHUNKS)), dma((m,)), dma((m,)), dma((n,)), dma((n,)),
            ],
            compiler_params=pltpu.CompilerParams(collective_id=0, has_side_effects=True),
        )(points, weights.reshape(1, rows), coverage.reshape(1, rows), cand_index, winners)

        def emit(gains_in, final_in, gains_out, final_out):
            gains_out[...] = gains_in[...]
            final_out[...] = final_in[...]

        gains, final = pl.pallas_call(
            emit,
            out_shape=(jax.ShapeDtypeStruct((iters, per_dev), jnp.float32),
                       jax.ShapeDtypeStruct((1, rows), jnp.float32)),
            in_specs=[vmem, vmem],
            out_specs=(vmem, vmem),
        )(gains, final)
        return gains, final.reshape(rows)

    return jax.shard_map(
        body,
        mesh=mesh,
        in_specs=(P("pts", None), P("pts"), P("pts"), P(None, "pts"), P()),
        out_specs=(P(None, ("pts", "cand")), P("pts")),
        check_vma=False,
    )
```

```python
import functools

import jax
import jax.numpy as jnp
from jax import lax
from jax.experimental import pallas as pl
from jax.experimental.pallas import tpu as pltpu
from jax.sharding import PartitionSpec as P

MESH = pl.DeviceIdType.MESH
CHUNKS = 8


def kernel(n, m, iters, per_dev, points_hbm, weight_ref, cover_ref, index_ref, winner_ref,
           gains_ref, final_ref, points, cands, sims, cols, parts, padded,
           load_sem, send_sem, recv_sem, col_send, col_recv, part_send, part_recv):
    me = lax.axis_index("pts")
    mine = lax.axis_index("cand")
    length = n // 4
    z = me // 4
    lane = me % 4
    x, y = lane % 2, lane // 2
    rows, width = points.shape
    block = iters * per_dev
    step_cols = width // CHUNKS
    scale = width ** (-0.5)

    load = pltpu.make_async_copy(points_hbm, points, load_sem)
    load.start()

    to_x = z * 4 + y * 2 + (1 - x)
    to_y = z * 4 + (1 - y) * 2 + x
    up, down = me + 4, me - 4
    has_up, has_down = z < length - 1, z > 0

    barrier = pltpu.get_barrier_semaphore()

    def greet(pts, cand):
        pl.semaphore_signal(barrier, inc=1, device_id=(pts, cand), device_id_type=MESH)

    greet(to_x, mine)
    greet(to_y, mine)
    for other in range(1, m):
        greet(me, lax.rem(mine + other, m))
    pl.when(has_up)(lambda: greet(up, mine))
    pl.when(has_down)(lambda: greet(down, mine))

    load.wait()
    place_row = lax.broadcasted_iota(jnp.int32, (block, rows), 0)
    place_col = lax.broadcasted_iota(jnp.int32, (block, rows), 1)
    choose = jnp.zeros((block, rows), jnp.float32)
    for t in range(iters):
        for k in range(per_dev):
            hit = place_col == index_ref[t, mine * per_dev + k]
            choose = jnp.where((place_row == t * per_dev + k) & hit, 1.0, choose)
    choose = choose.astype(jnp.bfloat16)
    for q in range(CHUNKS):
        span = slice(q * step_cols, (q + 1) * step_cols)
        cands[me, :, span] = jnp.dot(
            choose, points[:, span], preferred_element_type=jnp.float32).astype(jnp.bfloat16)

    pl.semaphore_wait(
        barrier, 2 + (m - 1) + has_up.astype(jnp.int32) + has_down.astype(jnp.int32))

    def columns(q):
        return pl.ds(pl.multiple_of(q * step_cols, 128), step_cols)

    def copy(p, q, way, target):
        part = cands.at[p, :, columns(q)]
        return pltpu.make_async_remote_copy(
            src_ref=part, dst_ref=part, send_sem=send_sem.at[p, way],
            recv_sem=recv_sem.at[p, q], device_id=(target, mine), device_id_type=MESH)

    last = length - 1
    middle = length // 2

    def direct(zp):
        return (zp >= middle) == (z >= middle)

    def routes(kind, zp):
        if kind == 0:
            return [(2, has_up & (zp <= z), up), (3, has_down & (zp >= z), down),
                    (0, None, to_x), (1, None, to_y)]
        if kind == 1:
            return [(1, direct(zp) & (zp % 2 == 1), to_y)]
        if kind == 2:
            return [(0, direct(zp) & (zp % 2 == 0), to_x)]
        return [(2, (zp < middle) & (z >= middle - 1) & has_up, up),
                (3, (zp >= middle) & (z <= middle) & has_down, down)]

    lanes = [lane, y * 2 + (1 - x), (1 - y) * 2 + x, (1 - y) * 2 + (1 - x)]

    def forward(kind, zp, q):
        p = zp * 4 + lanes[kind]
        for way, wanted, target in routes(kind, zp):
            def go(way=way, target=target):
                copy(p, q, way, target).start()
            if wanted is None:
                go()
            else:
                pl.when(wanted)(go)

    def settle(kind, zp):
        p = zp * 4 + lanes[kind]
        for way, wanted, target in routes(kind, zp):
            def go(way=way, target=target):
                pltpu.make_async_remote_copy(
                    src_ref=cands.at[p], dst_ref=cands.at[p], send_sem=send_sem.at[p, way],
                    recv_sem=recv_sem.at[p, 0], device_id=(target, mine),
                    device_id_type=MESH).wait_send()
            if wanted is None:
                go()
            else:
                pl.when(wanted)(go)

    for q in range(CHUNKS):
        forward(0, z, q)

    def stage(s, q):
        for kind, delay in ((0, 0), (1, 1), (2, 1), (3, 2)):
            for sign in (-1, 1):
                d = s - delay
                zp = z + sign * d
                valid = (zp >= 0) & (zp <= last) & (d >= (1 if kind == 0 or sign == 1 else 0))

                @pl.when(valid)
                def _(kind=kind, zp=zp):
                    copy(zp * 4 + lanes[kind], q, 0, to_x).wait_recv()
                    forward(kind, zp, q)

    def all_chunks(s, carry):
        lax.fori_loop(0, CHUNKS, lambda q, c: (stage(s, q), c)[1], 0)
        return carry

    lax.fori_loop(1, length + 1, all_chunks, 0)
    for q in range(CHUNKS):
        stage(length + 1, q)
        span = slice(q * step_cols, (q + 1) * step_cols)
        product = lax.dot_general(
            cands[:, :, span].reshape(n * block, step_cols), points[:, span],
            (((1,), (1,)), ((), ())), preferred_element_type=jnp.float32)
        if q == 0:
            sims[...] = product
        elif q < CHUNKS - 1:
            sims[...] += product
        else:
            sims[...] = (sims[...] + product) * scale

    def sim_of(t):
        return sims[...].reshape(n, iters, per_dev, rows)[:, t].reshape(n * per_dev, rows)

    place = lax.broadcasted_iota(jnp.int32, (n * per_dev, 1), 0)
    column = (place // per_dev) * (per_dev * m) + mine * per_dev + place % per_dev
    for t in range(iters):
        picked = jnp.where(column == winner_ref[t], sim_of(t), 0.0)
        cols[mine, t:t + 1, :] = jnp.sum(picked, axis=0, keepdims=True)

    def col_copy(slot, peer):
        return pltpu.make_async_remote_copy(
            src_ref=cols.at[slot], dst_ref=cols.at[slot], send_sem=col_send.at[peer],
            recv_sem=col_recv.at[slot], device_id=(me, peer), device_id_type=MESH)

    peers = [lax.rem(mine + other, m) for other in range(1, m)]
    for peer in peers:
        col_copy(mine, peer).start()

    weight = weight_ref[...]

    def gain(t, cover):
        terms = weight * jnp.maximum(sim_of(t) - cover, 0.0)
        folded = terms[:, 0:128]
        for g in range(1, rows // 128):
            folded = folded + terms[:, g * 128:(g + 1) * 128]
        return jnp.sum(folded.T, axis=0, keepdims=True)

    cover = cover_ref[...]
    for t in range(iters):
        parts[me, t:t + 1, :] = gain(t, cover)
        if t == 0:
            for peer in peers:
                col_copy(peer, peer).wait_recv()
        best = cols[0, t:t + 1, :]
        for c in range(1, m):
            best = best + cols[c, t:t + 1, :]
        cover = jnp.maximum(cover, best)

    def part_copy(slot, target):
        return pltpu.make_async_remote_copy(
            src_ref=parts.at[slot], dst_ref=parts.at[slot], send_sem=part_send.at[target],
            recv_sem=part_recv.at[slot], device_id=(target, mine), device_id_type=MESH)

    others = [lax.rem(me + other, n) for other in range(1, n)]
    for target in others:
        part_copy(me, target).start()
    final_ref[...] = cover

    settle(0, z)
    for kind in range(4):
        def each(zp, carry, kind=kind):
            if kind == 0:
                pl.when(zp != z)(lambda: settle(0, zp))
            else:
                settle(kind, zp)
            return carry
        lax.fori_loop(0, length, each, 0)
    for peer in peers:
        col_copy(mine, peer).wait_send()

    for source in others:
        part_copy(source, source).wait_recv()
    total = parts[0]
    for p in range(1, n):
        total = total + parts[p]
    padded[...] = jnp.zeros_like(padded)
    padded[0:iters, :] = total / float(rows * n)
    turned = pltpu.roll(padded[...], (n - me) * per_dev, 1)
    gains_ref[...] = turned[0:iters, 0:per_dev]
    for target in others:
        part_copy(me, target).wait_send()


def solution(mesh):
    n, m = mesh.shape["pts"], mesh.shape["cand"]

    def body(points, weights, coverage, cand_index, winners):
        rows, width = points.shape
        iters, per_row = cand_index.shape
        per_dev = per_row // m
        block = iters * per_dev
        vmem = pl.BlockSpec(memory_space=pltpu.VMEM)
        smem = pl.BlockSpec(memory_space=pltpu.SMEM)
        dma = pltpu.SemaphoreType.DMA
        gains, final = pl.pallas_call(
            functools.partial(kernel, n, m, iters, per_dev),
            out_shape=(jax.ShapeDtypeStruct((iters, per_dev), jnp.float32),
                       jax.ShapeDtypeStruct((1, rows), jnp.float32)),
            in_specs=[pl.BlockSpec(memory_space=pl.ANY), vmem, vmem, smem, smem],
            out_specs=(vmem, vmem),
            scratch_shapes=[
                pltpu.VMEM((rows, width), jnp.bfloat16),
                pltpu.VMEM((n, block, width), jnp.bfloat16),
                pltpu.VMEM((n * block, rows), jnp.float32),
                pltpu.VMEM((m, iters, rows), jnp.float32),
                pltpu.VMEM((n, iters, n * per_dev), jnp.float32),
                pltpu.VMEM((8, n * per_dev), jnp.float32),
                dma, dma((n, 4)), dma((n, CHUNKS)), dma((m,)), dma((m,)), dma((n,)), dma((n,)),
            ],
            compiler_params=pltpu.CompilerParams(collective_id=0, has_side_effects=True),
        )(points, weights.reshape(1, rows), coverage.reshape(1, rows), cand_index, winners)

        def emit(gains_in, final_in, gains_out, final_out):
            gains_out[...] = gains_in[...]
            final_out[...] = final_in[...]

        gains, final = pl.pallas_call(
            emit,
            out_shape=(jax.ShapeDtypeStruct((iters, per_dev), jnp.float32),
                       jax.ShapeDtypeStruct((1, rows), jnp.float32)),
            in_specs=[vmem, vmem],
            out_specs=(vmem, vmem),
        )(gains, final)
        return gains, final.reshape(rows)

    return jax.shard_map(
        body,
        mesh=mesh,
        in_specs=(P("pts", None), P("pts"), P("pts"), P(None, "pts"), P()),
        out_specs=(P(None, ("pts", "cand")), P("pts")),
        check_vma=False,
    )
```
